32 devices in a mesh: ep: 4 (over z), fsdp: 4 (over x, core), tp: 2 (over y).
Axes of the slice: x: 2, y: 2, z: 4, core: 2. Of those that a mesh axis runs over, the one named last changes fastest.
Arguments:
- out_grad: bfloat16 [2048, 4096], P(('ep', 'fsdp')), may hold values from -1.5 to 1.5
- routes: int32 [2048, 2], P(('ep', 'fsdp')), may hold values from 0 to 3, all different within a row; in each aligned block of 128 rows (0 to 127, 128 to 255, ...) at most 128 rows name the same one
- chosen_logits: float32 [2048, 2], P(('ep', 'fsdp')), may hold values from -4 to 4
- routed_inputs: bfloat16 [4, 4, 4, 128, 4096], P('ep', None, 'fsdp'), may hold values from -6 to 6
- w_gate: bfloat16 [4, 4096, 512], P('ep', 'fsdp', 'tp'), may hold values from -0.09375 to 0.09375
- w_up: bfloat16 [4, 4096, 512], P('ep', 'fsdp', 'tp'), may hold values from -0.09375 to 0.09375
- w_down: bfloat16 [4, 512, 4096], P('ep', 'tp', 'fsdp'), may hold values from -0.25 to 0.25
Outputs:
- input_grad: bfloat16 [2048, 4096], P(('ep', 'fsdp'))
- logit_grad: float32 [2048, 2], P(('ep', 'fsdp'))
- grad_gate: float32 [4, 4096, 512], P('ep', 'fsdp', 'tp')
- grad_up: float32 [4, 4096, 512], P('ep', 'fsdp', 'tp')
- grad_down: float32 [4, 512, 4096], P('ep', 'tp', 'fsdp')
The draws below stay inside these ranges and needn't reach their ends.
Inputs may be any that keep to these rules, and one draw needn't show every extreme that they name: Each row of routes names 2 different experts. In each token group of 128 consecutive rows no expert is named by more than 128 rows, a bound that some block reaches.
All inputs are finite; a program needn't handle non-finite values.
Results may differ from the reference program's by a relative error of at most 0.015.
Values may be sent and summed in bfloat16 or wider, within the bound.
A program may use at most 128 MiB of HBM per device.

```python
import math
import jax
import jax.numpy as jnp
import numpy as np
from jax import lax

D = 4096
TOP = 2
FF = 512
TOK_DEV = 128
EXPERTS = 4
SOURCES = 4
GROUPS = 4
CAPACITY = 128
TOKENS = 2048


def steps_of(key, extent, shards, least, top_value):
    factor_of = 1.0
    for axis_at, parts in shards:
        draws = jax.random.uniform(jax.random.fold_in(jax.random.fold_in(key, 6), axis_at), (parts,), jnp.float32, least / len(shards), top_value / len(shards))
        factor_of = factor_of * jnp.repeat(jnp.exp(draws), extent[axis_at] // parts).reshape((-1,) + (1,) * (len(extent) - 1 - axis_at))
    return factor_of


def shared_out(key, own, number, rows, amount, top, reach, skew):
    order = jax.random.permutation(key, amount)
    crowded, common = shares(amount, rows * top, reach, skew, True), shares(amount, rows * top, reach, skew, False)
    places = jnp.arange(amount)

    def named(sizes, rotation):
        used = int((sizes > 0).sum())
        fixed = max(1, used // 4)
        moved = fixed + (places - fixed + rotation * (used - fixed)) % max(1, amount - fixed)
        return jnp.zeros((amount,), jnp.int32).at[order[jnp.where(places < fixed, places, moved)]].set(jnp.asarray(sizes, jnp.int32))

    sizes = jnp.where(number % 4 == 0, named(crowded, number // 4), named(common, number - number // 4 - 1))
    mixed = jax.random.permutation(jax.random.fold_in(own, 3), amount)
    donor, receiver = mixed[0:amount // 2 * 2:2], mixed[1:amount // 2 * 2:2]
    room = jnp.minimum(sizes[donor] - 1, reach - sizes[receiver]) // 2
    room = jnp.where((donor == order[0]) | (receiver == order[0]) | (sizes[receiver] == 0), 0, jnp.maximum(room, 0))
    moved = jax.random.randint(jax.random.fold_in(own, 4), (amount // 2,), 0, 1 << 20) % (room + 1)
    sizes = sizes.at[donor].add(-moved).at[receiver].add(moved)
    labels = jnp.searchsorted(jnp.cumsum(sizes), jnp.arange(rows * top), side="right").astype(jnp.int32)
    grid = labels.reshape(top, rows).T
    grid = grid[jax.random.permutation(jax.random.fold_in(own, 1), rows)]
    rotation = jax.random.randint(jax.random.fold_in(own, 2), (rows, 1), 0, top)
    return jnp.take_along_axis(grid, (jnp.arange(top)[None, :] + rotation) % top, axis=1)


def shares(count, total, bound, slope, full):
    loads = [(1 << 20) // math.isqrt(standing ** slope) + 1 for standing in range(1, count + 1)]
    largest = bound if full else min(bound, max(-(-total // count), total * loads[0] // sum(loads)))
    least = 1 if total - largest >= count - 1 else 0
    holding, spare = [largest] + [least] * (count - 1), total - largest - least * (count - 1)
    while spare > 0:
        candidates = [i for i in range(1, count) if holding[i] < largest] or [i for i in range(1, count) if holding[i] < bound]
        mass, remaining = sum([loads[i] for i in candidates]), spare
        for i in candidates:
            more = min(bound - holding[i], max(1, remaining * loads[i] // mass), spare)
            holding[i] = holding[i] + more
            spare = spare - more
    return np.array(holding)


def scatter_about(own_key, dims, spread, reach, cuts=(), kind=jnp.bfloat16):
    drawn = jax.random.normal(own_key, dims, jnp.float32) * spread
    if len(cuts) > 0:
        drawn = steps_of(own_key, dims, cuts, -0.22, 0.18) * drawn
    return jnp.clip(drawn, min=-reach, max=reach).astype(kind)


def setup_inputs(seed: int = 0) -> dict:
    arg_keys = jax.random.split(jax.random.key(seed), 8)
    out_grad = scatter_about(arg_keys[0], (TOKENS, D), 0.25, 1.5, ((0, 16),))
    routes_keys = jax.random.split(jax.random.fold_in(arg_keys[1], 1), TOKENS // TOK_DEV)
    routes_turns = jax.random.permutation(jax.random.fold_in(arg_keys[1], 3), TOKENS // TOK_DEV)
    routes = jax.vmap(lambda own, number: shared_out(jax.random.fold_in(arg_keys[1], 2), own, number, TOK_DEV, EXPERTS, TOP, CAPACITY, 1))(routes_keys, routes_turns).reshape((TOKENS, TOP))
    chosen_logits = scatter_about(arg_keys[2], (TOKENS, TOP), 1.0, 4.0, ((0, 16),), jnp.float32)
    routed_inputs = scatter_about(arg_keys[3], (EXPERTS, SOURCES, GROUPS, CAPACITY, D), 1.0, 6.0, ((0, 4), (2, 4)))
    w_gate = scatter_about(arg_keys[4], (EXPERTS, D, FF), D ** -0.5, 0.09375, ((0, 4), (1, 4), (2, 2)))
    w_up = scatter_about(arg_keys[5], (EXPERTS, D, FF), D ** -0.5, 0.09375, ((0, 4), (1, 4), (2, 2)))
    w_down = scatter_about(arg_keys[6], (EXPERTS, FF, D), FF ** -0.5, 0.25, ((0, 4), (1, 2), (2, 4)))
    return dict(out_grad=out_grad, routes=routes, chosen_logits=chosen_logits, routed_inputs=routed_inputs, w_gate=w_gate, w_up=w_up, w_down=w_down)


def group_slots(routes):
    flat_routes = routes.reshape(-1, TOK_DEV * TOP)
    onehot = (flat_routes[:, :, None] == jnp.arange(EXPERTS, dtype=jnp.int32)[None, None, :]).astype(jnp.int32)
    earlier = (jnp.cumsum(onehot, axis=1) - onehot).astype(jnp.int32)
    position = jnp.sum(earlier * onehot, axis=2).astype(jnp.int32)
    return (flat_routes * CAPACITY + position).astype(jnp.int32)


def take_rows(row_values, row_index):
    return jnp.take(row_values, row_index, axis=0)


def expert_pass(operands):
    inputs, scaled, gate_weight, up_weight, down_weight = operands
    gate_act = jnp.dot(inputs, gate_weight, preferred_element_type=jnp.float32)
    up_act = jnp.dot(inputs, up_weight, preferred_element_type=jnp.float32)
    sigmoid_gate = jax.nn.sigmoid(gate_act)
    silu_gate = gate_act * sigmoid_gate
    hidden = (silu_gate * up_act).astype(jnp.bfloat16)
    hidden_grad = jnp.dot(scaled, down_weight.T, preferred_element_type=jnp.float32)
    products = jnp.sum(hidden_grad * hidden.astype(jnp.float32), axis=1).astype(jnp.bfloat16)
    up_grad = (hidden_grad * silu_gate).astype(jnp.bfloat16)
    gate_grad = (hidden_grad * up_act * sigmoid_gate * (1.0 + gate_act * (1.0 - sigmoid_gate))).astype(jnp.bfloat16)
    grad_gate = jnp.dot(inputs.T, gate_grad, preferred_element_type=jnp.float32)
    grad_up = jnp.dot(inputs.T, up_grad, preferred_element_type=jnp.float32)
    grad_down = jnp.dot(hidden.T, scaled, preferred_element_type=jnp.float32)
    slot_grad = jnp.dot(gate_grad, gate_weight.T, preferred_element_type=jnp.float32)
    slot_grad = (slot_grad + jnp.dot(up_grad, up_weight.T, preferred_element_type=jnp.float32)).astype(jnp.bfloat16)
    return grad_gate, grad_up, grad_down, slot_grad, products


def reference(out_grad, routes, chosen_logits, routed_inputs, w_gate, w_up, w_down):
    groups = TOKENS // TOK_DEV
    pair_count = TOK_DEV * TOP
    gate_probs = jax.nn.softmax(chosen_logits, axis=-1)
    slot_index = group_slots(routes)
    weighted = (gate_probs[:, :, None] * out_grad.astype(jnp.float32)[:, None, :]).astype(jnp.bfloat16)
    weighted = weighted.reshape(groups, pair_count, D)
    weighted = jnp.concatenate([weighted, jnp.zeros((groups, 1, D), jnp.bfloat16)], axis=1)
    source = jnp.full((groups, EXPERTS * CAPACITY), pair_count, jnp.int32)
    group_rows = jnp.arange(groups, dtype=jnp.int32)[:, None]
    pair_ids = jnp.broadcast_to(jnp.arange(pair_count, dtype=jnp.int32)[None, :], (groups, pair_count))
    source = source.at[group_rows, slot_index].set(pair_ids)
    scaled = jax.vmap(take_rows)(weighted, source)
    scaled = scaled.reshape(groups, EXPERTS, CAPACITY, D).transpose(1, 0, 2, 3).reshape(EXPERTS, groups * CAPACITY, D)
    inputs = routed_inputs.reshape(EXPERTS, groups * CAPACITY, D)
    grad_gate, grad_up, grad_down, slot_grad, products = lax.map(expert_pass, (inputs, scaled, w_gate, w_up, w_down))
    slot_grad = slot_grad.reshape(EXPERTS, groups, CAPACITY, D).transpose(1, 0, 2, 3).reshape(groups, EXPERTS * CAPACITY, D)
    picked = jax.vmap(take_rows)(slot_grad, slot_index).astype(jnp.float32)
    input_grad = jnp.sum(picked.reshape(TOKENS, TOP, D), axis=1).astype(jnp.bfloat16)
    products = products.reshape(EXPERTS, groups, CAPACITY).transpose(1, 0, 2).reshape(groups, EXPERTS * CAPACITY)
    chosen = jnp.take_along_axis(products, slot_index, axis=1).astype(jnp.float32).reshape(TOKENS, TOP)
    logit_grad = chosen - gate_probs * jnp.sum(chosen, axis=1, keepdims=True)
    return (input_grad, logit_grad, grad_gate, grad_up, grad_down)
```

```python
import functools

import jax
import jax.numpy as jnp
from jax import lax
from jax.experimental import pallas as pl
from jax.experimental.pallas import tpu as pltpu
from jax.sharding import PartitionSpec as P

MESH = pl.DeviceIdType.MESH
AXES = ("ep", "fsdp", "tp")


def when(cond, fn):
    pl.when(cond)(fn)


def entry_barrier():
    barrier = pltpu.get_barrier_semaphore()
    for axis in AXES:
        size, me = lax.axis_size(axis), lax.axis_index(axis)
        for step in range(1, size):
            if step not in (1, size - 1) and axis != "tp":
                continue
            peer = lax.rem(me + step, size)
            pl.semaphore_signal(barrier, inc=1, device_id={axis: peer}, device_id_type=MESH)
    count = 0
    for axis in AXES:
        size = lax.axis_size(axis)
        count += size - 1 if axis == "tp" else min(2, size - 1)
    pl.semaphore_wait(barrier, count)


def gather_kernel(
    rows_ref, meta_ref, gate_ref, up_ref, down_ref,
    rows_out, meta_out, gate_out, up_out, down_out,
    send_sem, recv_sem, fsend_sem, frecv_sem, tsend_sem, trecv_sem,
):
    ep, fs, tp = (lax.axis_index(a) for a in AXES)
    n_ep, n_fs, n_tp = (lax.axis_size(a) for a in AXES)
    width = rows_ref.shape[1] // n_tp
    depth = down_ref.shape[1]

    def cols(k):
        return pl.ds(pl.multiple_of(k * width, width), width)

    def chunk(k):
        return pl.ds(pl.multiple_of(k * depth, depth), depth)

    ep_streams = (
        (rows_ref.at[:, cols(tp)], lambda b: rows_out.at[b, :, cols(tp)]),
        (meta_ref, lambda b: meta_out.at[b]),
    )
    fs_streams = (
        (gate_ref, lambda b: gate_out.at[b]),
        (up_ref, lambda b: up_out.at[b]),
        (down_ref, lambda b: down_out.at[:, chunk(b)]),
    )

    def copy(axis, index, stream, block, own, way, peer):
        source, place = stream
        sends, recvs = (send_sem, recv_sem) if axis == "ep" else (fsend_sem, frecv_sem)
        return pltpu.make_async_remote_copy(
            src_ref=source if own else place(block),
            dst_ref=place(block),
            send_sem=sends.at[index, way, block],
            recv_sem=recvs.at[index, block],
            device_id={axis: peer},
            device_id_type=MESH,
        )

    def tp_copy(block, step, owner, peer):
        return pltpu.make_async_remote_copy(
            src_ref=rows_out.at[block, :, cols(owner)],
            dst_ref=rows_out.at[block, :, cols(owner)],
            send_sem=tsend_sem.at[block, step],
            recv_sem=trecv_sem.at[block, step],
            device_id={"tp": peer},
            device_id_type=MESH,
        )

    entry_barrier()

    def advance(axis, me, size, streams, r, finish):
        for way, sign in ((0, 1), (1, -1)):
            block = me - sign * r
            have = jnp.logical_and(block >= 0, block < size)
            peer = me + sign
            more = jnp.logical_and(peer >= 0, peer < size)
            for index, stream in enumerate(streams):
                if not finish and r > 0:
                    def arrived(index=index, stream=stream):
                        copy(axis, index, stream, block, False, way, me - sign).wait_recv()
                        if axis == "ep" and index == 0:
                            for step in range(1, n_tp):
                                tp_copy(block, step - 1, tp, lax.rem(tp + step, n_tp)).start()
                    when(have, arrived)

                if r < size - 1:
                    def send(index=index, stream=stream):
                        c = copy(axis, index, stream, block, r == 0, way, peer)
                        if finish:
                            c.wait_send()
                        else:
                            c.start()
                    when(jnp.logical_and(have, more), send)

    for finish in (False, True):
        for r in range(max(n_ep, n_fs)):
            if r < n_ep:
                advance("ep", ep, n_ep, ep_streams, r, finish)
            if r < n_fs:
                advance("fsdp", fs, n_fs, fs_streams, r, finish)
            if r == 0 and not finish:
                rows_out[ep] = rows_ref[...]
                meta_out[ep] = meta_ref[...]
                gate_out[fs] = gate_ref[...]
                up_out[fs] = up_ref[...]
                down_out[:, chunk(fs)] = down_ref[...]
    for block in range(n_ep):
        def close(block=block):
            for step in range(1, n_tp):
                tp_copy(block, step - 1, tp, lax.rem(tp + step, n_tp)).wait_send()
                owner = lax.rem(tp + n_tp - step, n_tp)
                tp_copy(block, step - 1, owner, owner).wait_recv()
        when(block != ep, close)


def gather_all(rows, meta, gate, up, down):
    n_ep, n_fs, n_tp = (lax.axis_size(a) for a in AXES)
    vmem = pl.BlockSpec(memory_space=pltpu.VMEM)
    dma = pltpu.SemaphoreType.DMA
    return pl.pallas_call(
        gather_kernel,
        out_shape=(
            jax.ShapeDtypeStruct((n_ep, *rows.shape), rows.dtype),
            jax.ShapeDtypeStruct((n_ep, *meta.shape), meta.dtype),
            jax.ShapeDtypeStruct((n_fs, *gate.shape), gate.dtype),
            jax.ShapeDtypeStruct((n_fs, *up.shape), up.dtype),
            jax.ShapeDtypeStruct((down.shape[0], n_fs * down.shape[1]), down.dtype),
        ),
        in_specs=[vmem] * 5,
        out_specs=[vmem] * 5,
        scratch_shapes=[
            dma((2, 2, n_ep)),
            dma((2, n_ep)),
            dma((3, 2, n_fs)),
            dma((3, n_fs)),
            dma((n_ep, max(1, n_tp - 1))),
            dma((n_ep, max(1, n_tp - 1))),
        ],
        compiler_params=pltpu.CompilerParams(
            collective_id=0, has_side_effects=True, vmem_limit_bytes=48 * 1024 * 1024
        ),
    )(rows, meta, gate, up, down)


def transpose_dot(left, right):
    return lax.dot_general(
        left, right, (((0,), (0,)), ((), ())), preferred_element_type=jnp.float32
    )


def contract_last(left, right):
    return lax.dot_general(
        left, right, (((1,), (1,)), ((), ())), preferred_element_type=jnp.float32
    )


def body(out_grad, routes, chosen_logits, routed_inputs, w_gate, w_up, w_down):
    groups = lax.axis_size("ep")
    me = lax.axis_index("ep")
    tokens, model_width = out_grad.shape
    per_token = routes.shape[1]
    capacity = routed_inputs.shape[3]
    inputs = routed_inputs.reshape(-1, model_width)
    own_probs = jax.nn.softmax(chosen_logits, axis=-1)
    meta = jnp.concatenate(
        [
            routes.astype(jnp.float32).T,
            own_probs.T,
            jnp.zeros((8 - 2 * per_token, tokens), jnp.float32),
        ],
        axis=0,
    )
    rows, meta_all, gate_full, up_full, down_full = gather_all(
        out_grad, meta, w_gate[0], w_up[0], w_down[0]
    )
    gate_full = gate_full.reshape(model_width, -1)
    up_full = up_full.reshape(model_width, -1)
    chosen_here = (meta_all[:, :per_token] == me.astype(jnp.float32)).astype(jnp.float32)
    weight = jnp.sum(chosen_here * meta_all[:, per_token : 2 * per_token], axis=1)
    mask = jnp.sum(chosen_here, axis=1)
    order = jnp.arange(tokens)
    earlier = (order[:, None] < order[None, :]).astype(jnp.bfloat16)
    place = jnp.dot(mask.astype(jnp.bfloat16), earlier, preferred_element_type=jnp.float32)
    hit = (place[:, None, :] == jnp.arange(capacity, dtype=jnp.float32)[None, :, None]) & (
        mask[:, None, :] > 0
    )
    select = hit.astype(jnp.bfloat16)
    slot_weight = jnp.sum(jnp.where(hit, weight[:, None, :], 0.0), axis=2)
    picked = lax.dot_general(
        select, rows, (((2,), (1,)), ((0,), (0,))), preferred_element_type=jnp.float32
    )
    scaled = (picked * slot_weight[:, :, None]).astype(jnp.bfloat16).reshape(-1, model_width)

    gate_act = jnp.dot(inputs, gate_full, preferred_element_type=jnp.float32)
    up_act = jnp.dot(inputs, up_full, preferred_element_type=jnp.float32)
    sigmoid_gate = jax.nn.sigmoid(gate_act)
    silu_gate = gate_act * sigmoid_gate
    hidden = (silu_gate * up_act).astype(jnp.bfloat16)
    hidden_grad = contract_last(scaled, down_full)
    products = jnp.sum(hidden_grad * hidden.astype(jnp.float32), axis=1)
    up_grad = (hidden_grad * silu_gate).astype(jnp.bfloat16)
    gate_grad = (
        hidden_grad * up_act * sigmoid_gate * (1.0 + gate_act * (1.0 - sigmoid_gate))
    ).astype(jnp.bfloat16)
    pair_grads = jnp.concatenate([gate_grad, up_grad], axis=1)
    hidden_units = hidden.shape[1]
    pair_rows = lax.dot_general(
        select,
        pair_grads.reshape(groups, capacity, -1),
        (((1,), (1,)), ((0,), (0,))),
        preferred_element_type=jnp.float32,
    ).astype(jnp.bfloat16).reshape(groups * tokens, -1)
    token_part = contract_last(pair_rows[:, :hidden_units], gate_full) + contract_last(
        pair_rows[:, hidden_units:], up_full
    )
    column_sum = lax.psum_scatter(
        token_part.astype(jnp.bfloat16), "tp", scatter_dimension=1, tiled=True
    )
    combined = lax.psum_scatter(column_sum, "ep", scatter_dimension=0, tiled=True)
    input_grad = lax.all_gather(combined, "tp", axis=1, tiled=True)

    token_products = jnp.sum(
        jnp.where(hit, products.reshape(groups, capacity)[:, :, None], 0.0), axis=1
    )
    pair_products = chosen_here * token_products[:, None, :]
    product_sum = lax.psum(pair_products, ("ep", "tp"))
    chosen = lax.dynamic_index_in_dim(product_sum, me, 0, keepdims=False).T
    chosen = lax.reduce_precision(chosen, 8, 7)
    logit_grad = chosen - own_probs * jnp.sum(chosen, axis=1, keepdims=True)

    gate_up = transpose_dot(inputs, pair_grads)
    down_part = transpose_dot(scaled, hidden)
    whole = jnp.concatenate([gate_up, down_part], axis=1).astype(jnp.bfloat16)
    grad_rows = lax.psum_scatter(whole, "fsdp", scatter_dimension=0, tiled=True).astype(
        jnp.float32
    )
    grad_gate = grad_rows[:, :hidden_units][None]
    grad_up = grad_rows[:, hidden_units : 2 * hidden_units][None]
    grad_down = grad_rows[:, 2 * hidden_units :].T[None]
    return (input_grad, logit_grad, grad_gate, grad_up, grad_down)


def solution(mesh):
    in_specs = (
        P(("ep", "fsdp"), None),
        P(("ep", "fsdp"), None),
        P(("ep", "fsdp"), None),
        P("ep", None, "fsdp", None, None),
        P("ep", "fsdp", "tp"),
        P("ep", "fsdp", "tp"),
        P("ep", "tp", "fsdp"),
    )
    out_specs = (
        P(("ep", "fsdp"), None),
        P(("ep", "fsdp"), None),
        P("ep", "fsdp", "tp"),
        P("ep", "fsdp", "tp"),
        P("ep", "tp", "fsdp"),
    )
    return jax.shard_map(body, mesh=mesh, in_specs=in_specs, out_specs=out_specs, check_vma=False)
```
